32 devices in a mesh: scene: 2 (over x), az: 16 (over z, y, core).
Axes of the slice: x: 2, y: 2, z: 4, core: 2. Of those that a mesh axis runs over, the one named last changes fastest.
Arguments:
- secondary: bfloat16 [2, 512, 12288], P(None, ('scene', 'az')), parts along dimension 1, may hold values from -6 to 6
- line_valid: int32 [512], P(('scene', 'az')), parts along dimension 0, may hold values 0 or 1
- first_valid: int32 [512], P(('scene', 'az')), parts along dimension 0, may hold values from 0 to 3071
- last_valid: int32 [512], P(('scene', 'az')), parts along dimension 0, may hold values from 9216 to 12288
- az_coef: float32 [3, 512], P(None, ('scene', 'az')), parts along dimension 1, may hold values from -0.33 to 0.33
- az_base: int32 [512], P(('scene', 'az')), parts along dimension 0, may hold values from -3 to 3
- rg_base: int32 [512], P(('scene', 'az')), parts along dimension 0, may hold values from -8 to 8
- rg_coef: float32 [8], P('scene'), parts along dimension 0, may hold values from -3 to 3
- block_dest: int32 [512], P(('scene', 'az')), parts along dimension 0, may hold values from 0 to 255, as said below
Outputs:
- coreg: bfloat16 [2, 512, 12288], P(None, ('scene', 'az')), parts along dimension 1
- mean_power: float32 [2], P('scene'), parts along dimension 0
- valid_share: float32 [2], P('scene'), parts along dimension 0
The draws below stay inside these ranges and needn't reach their ends.
There are 2 independent parts, one for each index of `scene`. The reference program is written for one: setup_inputs(seed, part) draws one part's arguments, and reference() takes and returns one part's arrays. A program takes and returns all parts, laid end to end along the dimension named above; each array names one. Nothing has to cross between parts.
Inputs may be any that keep to these rules, and one draw needn't show every extreme that they name: `block_dest`: A permutation of 0 to 255. The 16 line blocks of each device of az take exactly one place on every device of az, itself included (place // 16 runs over all devices).
All inputs are finite; a program needn't handle non-finite values. No bound on the sum of `line_valid` on one device may be relied on, other than what follows from the above.
Results may differ from the reference program's by a relative error of at most 0.0066.
Values may be sent and summed in bfloat16 or wider, within the bound.
A program may use at most 128 MiB of HBM per device.

```python
import jax
import jax.numpy as jnp
from jax import lax

LINES = 1
RG = 12288
ABASE = 3
RBMAX = 8
HALO = 7
BLK_DEV = 16
AZ = 256
NBLK = 256


def draw_secondary(key, part):
    first_key, second_key = jax.random.split(key)
    values = jax.random.normal(first_key, (2, AZ, RG), jnp.float32)
    return jnp.clip(values, -6.0, 6.0).astype(jnp.bfloat16)


def draw_block_dest(key, part):
    blocks = BLK_DEV
    first_key, second_key = jax.random.split(key)
    offsets = jax.vmap(lambda inner_key: jax.random.permutation(inner_key, blocks))(jax.random.split(first_key, blocks))
    places = jax.vmap(lambda inner_key: jax.random.permutation(inner_key, blocks))(jax.random.split(second_key, blocks))
    source = jnp.broadcast_to(jnp.arange(blocks)[:, None], (blocks, blocks))
    target = (source + offsets) % blocks
    slot_at = places[target, source]
    return (target * blocks + slot_at).reshape(-1).astype(jnp.int32)


def touch_ends(array, stream_key, least, top_value):
    dims = array.shape
    index_at = [jax.random.randint(jax.random.fold_in(stream_key, axis), (), 0, dims[axis]) for axis in range(len(dims))]
    array = array.at[tuple(index_at)].set(least)
    longest = dims.index(max(dims))
    index_at[longest] = (index_at[longest] + 1) % dims[longest]
    return array.at[tuple(index_at)].set(top_value)


def block_levels(own_key, dims, cuts, low, largest):
    factor_of, own = 1.0, jax.random.fold_in(own_key, 6)
    for dim, parts in cuts:
        draws = jnp.exp(jax.random.uniform(jax.random.fold_in(own, dim), (parts,), jnp.float32, low / len(cuts), largest / len(cuts)))
        factor_of = factor_of * jnp.repeat(draws, dims[dim] // parts).reshape([-1 if axis == dim else 1 for axis in range(len(dims))])
    return factor_of


def setup_inputs(seed: int = 0, part: int = 0) -> dict:
    key_list = jax.random.split(jax.random.key(seed), 10)
    own_keys = jax.random.split(jax.random.fold_in(key_list[9], part), 10)
    return {
        "secondary": draw_secondary(jax.random.fold_in(jax.random.fold_in(key_list[9], part), 71), part),
        "line_valid": touch_ends((jax.random.randint(own_keys[1], (AZ,), 0, 4) < 3).astype(jnp.int32), jax.random.fold_in(own_keys[1], 1), 0, 1),
        "first_valid": touch_ends(jax.random.randint(own_keys[2], (AZ,), 0, RG // 4), jax.random.fold_in(own_keys[2], 1), 0, (RG // 4) - 1).astype(jnp.int32),
        "last_valid": touch_ends(jax.random.randint(own_keys[3], (AZ,), RG - RG // 4, RG + 1), jax.random.fold_in(own_keys[3], 1), RG - RG // 4, RG).astype(jnp.int32),
        "az_coef": jnp.clip(jax.random.uniform(own_keys[4], (3, NBLK), jnp.float32, -0.33, 0.33) * block_levels(own_keys[4], (3, NBLK), ((1, 16),), -0.4, 0.0), -0.33, 0.33),
        "az_base": touch_ends(jax.random.randint(own_keys[5], (NBLK,), -ABASE, ABASE + 1), jax.random.fold_in(own_keys[5], 1), -ABASE, ABASE).astype(jnp.int32),
        "rg_base": touch_ends(jax.random.randint(own_keys[6], (NBLK,), -RBMAX, RBMAX + 1), jax.random.fold_in(own_keys[6], 1), -RBMAX, RBMAX).astype(jnp.int32),
        "rg_coef": jnp.clip(jax.random.uniform(own_keys[7], (4,), jnp.float32, -3.0, 3.0), -3.0, 3.0),
        "block_dest": draw_block_dest(jax.random.fold_in(jax.random.fold_in(key_list[9], part), 71), part),
    }


def sinc_taper(distance):
    in_reach = jnp.abs(distance) < 4.0
    shaped = jnp.sinc(distance) * (0.5 + 0.5 * jnp.cos(jnp.pi * distance / 4.0))
    return jnp.where(in_reach, shaped, jnp.zeros_like(distance))

def tap_weights(az_coef, line_count):
    position = (jnp.arange(line_count, dtype=jnp.float32) + 0.5) / line_count
    fraction = az_coef[0][:, None] + az_coef[1][:, None] * position + az_coef[2][:, None] * position * position
    tap_offsets = jnp.arange(9, dtype=jnp.float32) - 4.0
    return sinc_taper(tap_offsets[None, None, :] - fraction[:, :, None]).astype(jnp.bfloat16)

def range_tiles(rg_coef, col_count):
    tile_total = col_count // 128
    col_index = jnp.arange(col_count, dtype=jnp.float32)
    along = (col_index + 0.5) / col_count
    offsets = rg_coef[0] + rg_coef[1] * along + rg_coef[2] * along * along + rg_coef[3] * along * along * along
    offsets = offsets.reshape(tile_total, 128)
    inner = jnp.arange(128, dtype=jnp.float32)
    tile_gaps = (jnp.arange(3, dtype=jnp.float32) - 1.0) * 128.0
    distance = tile_gaps[:, None, None, None] + inner[None, None, :, None] - inner[None, None, None, :] - offsets[None, :, None, :]
    return sinc_taper(distance).astype(jnp.bfloat16)

def resample(windows, weights, kernel):
    line_count = weights.shape[1]
    summed = jnp.zeros(windows.shape[:2] + (line_count, windows.shape[3]), jnp.float32)
    for tap_index in range(9):
        summed = summed + weights[:, None, :, tap_index, None].astype(jnp.float32) * windows[:, :, tap_index:tap_index + line_count, :].astype(jnp.float32)
    azimuthal = summed.astype(jnp.bfloat16)
    col_count = azimuthal.shape[3]
    tile_total = col_count // 128
    tiled_rows = azimuthal.reshape(azimuthal.shape[:3] + (tile_total, 128))
    padded = jnp.pad(tiled_rows, ((0, 0), (0, 0), (0, 0), (1, 1), (0, 0)))
    ranged = jnp.zeros(tiled_rows.shape, jnp.float32)
    for shift_tile in range(3):
        ranged = ranged + jnp.einsum('bclti,tij->bcltj', padded[:, :, :, shift_tile:shift_tile + tile_total].astype(jnp.float32), kernel[shift_tile].astype(jnp.float32))
    return ranged.reshape(azimuthal.shape).astype(jnp.bfloat16)

def reference(secondary, line_valid, first_valid, last_valid, az_coef, az_base, rg_base, rg_coef, block_dest):
    col_index = jnp.arange(RG, dtype=jnp.int32)
    kept_mask = (line_valid[:, None] > 0) & (col_index[None, :] >= first_valid[:, None]) & (col_index[None, :] < last_valid[:, None])
    masked = jnp.where(kept_mask[None], secondary, jnp.zeros((), jnp.bfloat16))
    valid_total = jnp.sum(kept_mask.astype(jnp.int32)).astype(jnp.float32)
    padded = jnp.pad(masked, ((0, 0), (HALO, HALO), (RBMAX, RBMAX)))
    weights = tap_weights(az_coef, LINES)
    kernel = range_tiles(rg_coef, RG)
    row_starts = (jnp.arange(NBLK, dtype=jnp.int32) * LINES + az_base - 4 + HALO).astype(jnp.int32)
    col_starts = (RBMAX + rg_base).astype(jnp.int32)

    def one_group(group_index):
        first_block = (group_index * BLK_DEV).astype(jnp.int32)
        rows_here = lax.dynamic_slice_in_dim(row_starts, first_block, BLK_DEV)
        cols_here = lax.dynamic_slice_in_dim(col_starts, first_block, BLK_DEV)
        windows = jax.vmap(lambda rows_at, cols_at: lax.dynamic_slice(padded, (jnp.int32(0), rows_at, cols_at), (2, LINES + 8, RG)))(rows_here, cols_here)
        group_weights = lax.dynamic_slice_in_dim(weights, first_block, BLK_DEV)
        return resample(windows, group_weights, kernel)
    resampled_groups = lax.map(one_group, jnp.arange(NBLK // BLK_DEV, dtype=jnp.int32))
    resampled = resampled_groups.reshape(NBLK, 2, LINES, RG)
    total_power = jnp.sum(jnp.square(resampled.astype(jnp.float32)))
    mean_power = total_power / jnp.maximum(valid_total, 1.0)
    power_gain = lax.rsqrt(mean_power + 0.5)
    scaled = (resampled.astype(jnp.float32) * power_gain).astype(jnp.bfloat16)
    placed = jnp.zeros_like(scaled).at[block_dest].set(scaled)
    coreg = jnp.moveaxis(placed, 1, 0).reshape(2, AZ, RG)
    valid_share = valid_total / (AZ * RG)
    return (coreg, mean_power.reshape(1), valid_share.reshape(1))
```

```python
import functools

import jax
import jax.numpy as jnp
from jax import lax
from jax.experimental import pallas as pl
from jax.experimental.pallas import tpu as pltpu
from jax.sharding import PartitionSpec as P

HALO = 8
TAPS = 11
PAD = 8
META = 16
PI = 3.141592653589793


def sinc_taper(distance):
    in_reach = jnp.abs(distance) < 4.0
    shaped = jnp.sinc(distance) * (0.5 + 0.5 * jnp.cos(jnp.pi * distance / 4.0))
    return jnp.where(in_reach, shaped, jnp.zeros_like(distance))


def azimuth_band(az_coef, az_base):
    blocks = az_base.shape[0]
    q = 0.5
    fraction = az_coef[0] + az_coef[1] * q + az_coef[2] * q * q
    held = jnp.arange(blocks + 2 * HALO, dtype=jnp.int32)
    own, low = held, held - blocks - HALO
    high = held - HALO
    row = jnp.where(held < blocks, own, jnp.where(held < blocks + HALO, low, high))
    gap = row[None, :] - jnp.arange(blocks, dtype=jnp.int32)[:, None] - az_base[:, None]
    value = sinc_taper(gap.astype(jnp.float32) - fraction[:, None])
    return jnp.where(jnp.abs(gap) <= 4, value, 0.0).astype(jnp.bfloat16)


def split3(x):
    hi = x.astype(jnp.bfloat16).astype(jnp.float32)
    rest = x - hi
    mid = rest.astype(jnp.bfloat16).astype(jnp.float32)
    return hi, mid, rest - mid


def filter_kernel(
    coef, shift, dest, valid, first, last, band, mid, low, high, sent, dense, weight, start
):
    blocks, cols = mid.shape[1], mid.shape[2]
    tiles = cols // 128
    groups = tiles // 8
    span = tiles + 2 * PAD

    for g in range(groups):
        centre = (g * 1024 + 512) / cols
        oc = coef[0] + coef[1] * centre + coef[2] * (centre * centre) + coef[3] * (centre**3)
        n0 = (oc - 5.0 + 64.0).astype(jnp.int32) - 63
        start[g] = n0
        sub = lax.broadcasted_iota(jnp.int32, (8, 128), 0)
        lane = lax.broadcasted_iota(jnp.int32, (8, 128), 1)
        col = g * 1024 + sub * 128 + lane
        v = (col.astype(jnp.float32) + 0.5) / cols
        off = coef[0] + coef[1] * v + coef[2] * v * v + coef[3] * v * v * v
        whole = jnp.round(off)
        part = off - whole
        odd = (whole.astype(jnp.int32) + n0) & 1
        sine = jnp.sin(PI * part) * (-1.0 / PI) * (1 - 2 * odd).astype(jnp.float32)
        base = (n0.astype(jnp.float32) - off) * (PI / 4.0)
        c0, s0 = jnp.cos(base), jnp.sin(base)
        for k in range(TAPS):
            n = n0 + k
            d = n.astype(jnp.float32) - off
            ck, sk = COS8[k % 8], COS8[(k - 2) % 8]
            taper = 0.5 + 0.5 * (c0 * ck - s0 * sk)
            top = sine if k % 2 == 0 else -sine
            near = d == 0.0
            val = jnp.where(near, 1.0, top / jnp.where(near, 1.0, d)) * taper
            keep = (jnp.abs(d) < 4.0) & (col + n >= 0) & (col + n < cols)
            val = jnp.where(keep, val, 0.0)
            weight[g, k] = val.astype(jnp.bfloat16).astype(jnp.float32)

    zero = jnp.zeros((PAD, 128), jnp.float32)

    def clear(r, carry):
        dense[pl.ds(pl.multiple_of(r * span, 8), PAD), :] = zero
        dense[pl.ds(pl.multiple_of(r * span + PAD + tiles, 8), PAD), :] = zero
        return carry

    lax.fori_loop(0, 2 * blocks, clear, 0)
    weights_az = band[...]
    for p in range(2):

        def azimuth(i, carry):
            at = pl.ds(pl.multiple_of(i * 512, 512), 512)
            rows = jnp.concatenate([mid[p, :, at], low[p, :, at], high[p, :, at]], axis=0)
            out = jnp.dot(weights_az, rows, preferred_element_type=jnp.float32)
            out = out.astype(jnp.bfloat16).astype(jnp.float32)
            for u in range(4):
                place = p * blocks * span + PAD + i * 4 + u
                dense[pl.ds(place, blocks, stride=span), :] = out[:, u * 128 : u * 128 + 128]
            return carry

        lax.fori_loop(0, tiles // 4, azimuth, 0)

    lane = lax.broadcasted_iota(jnp.int32, (8, 128), 1)

    def group(big, power):
        def line(j, power):
            to = dest[j] // blocks
            for p in range(2):
                halves = []
                for h in range(2):
                    g = big * 2 + h
                    b = shift[j] + start[g]
                    q = jnp.where(b < 0, 1, 0)
                    b = b + 128 * q
                    at = (p * blocks + j) * span + PAD + g * 8 - q
                    x0 = dense[pl.ds(at, 8), :]
                    x1 = dense[pl.ds(at + 1, 8), :]
                    x2 = dense[pl.ds(at + 2, 8), :]
                    under = lane < b
                    back = 128 - b
                    y0 = pltpu.roll(jnp.where(under, x1, x0), back, 1)
                    y1 = pltpu.roll(jnp.where(under, x2, x1), back, 1)
                    acc = weight[g, 0] * y0
                    for k in range(1, TAPS):
                        moved = pltpu.roll(jnp.where(lane < k, y1, y0), 128 - k, 1)
                        acc = acc + weight[g, k] * moved
                    halves.append(acc)
                done = jnp.concatenate(halves, axis=0).astype(jnp.bfloat16)
                sent[to, pl.ds(pl.multiple_of(p * tiles + big * 16, 16), 16), :] = done
                wide = done.astype(jnp.float32)
                power = power + wide * wide
            return power

        return lax.fori_loop(0, blocks, line, power, unroll=2)

    power = lax.fori_loop(0, tiles // 16, group, jnp.zeros((16, 128), jnp.float32))
    own_power = jnp.broadcast_to(jnp.sum(power, keepdims=True), (META, 128))
    count = jnp.int32(0)
    for j in range(blocks):
        have = jnp.minimum(last[j], cols) - jnp.maximum(first[j], 0)
        count = count + jnp.where(valid[j] > 0, jnp.maximum(have, 0), 0)
    own_count = jnp.full((META, 128), count, jnp.int32).astype(jnp.float32)
    row = lax.broadcasted_iota(jnp.int32, (META, 128), 0)
    meta = jnp.zeros((META, 128), jnp.float32)
    for i, piece in enumerate(split3(own_power) + split3(own_count)):
        meta = jnp.where(row == i + 1, piece, meta)
    for j in range(blocks):
        place = jnp.full((META, 128), dest[j] % blocks, jnp.int32).astype(jnp.float32)
        note = jnp.where(row == 0, place, meta).astype(jnp.bfloat16)
        sent[dest[j] // blocks, pl.ds(2 * tiles, META), :] = note


HALF = 0.7071067811865476
COS8 = (1.0, HALF, 0.0, -HALF, -1.0, -HALF, 0.0, HALF)


def finish_kernel(total, got, out, mean, share, wide):
    blocks, cols = out.shape[1], out.shape[2]
    tiles = cols // 128
    notes = [got[s, pl.ds(2 * tiles, META), :].astype(jnp.float32) for s in range(blocks)]
    both = functools.reduce(lambda a, b: a + b, notes)
    power = both[1:2] + both[2:3] + both[3:4]
    count = both[4:5] + both[5:6] + both[6:7]
    mean_power = power / jnp.maximum(count, 1.0)
    gain = lax.rsqrt(mean_power + 0.5)
    mean[0] = mean_power[0, 0]
    share[0] = (count / float(total))[0, 0]
    for s in range(blocks):
        place = notes[s][0, 0].astype(jnp.int32)
        for p in range(2):
            x = got[s, pl.ds(p * tiles, tiles), :].astype(jnp.float32) * gain
            wide[pl.ds(pl.multiple_of((p * blocks + place) * tiles, 8), tiles), :] = x

    def tile(t, carry):
        at = pl.ds(pl.multiple_of(t * 128, 128), 128)
        for p in range(2):
            x = wide[pl.ds(p * blocks * tiles + t, blocks, stride=tiles), :]
            out[p, :, at] = x.astype(jnp.bfloat16)
        return carry

    lax.fori_loop(0, tiles, tile, 0, unroll=8)


def shards(
    secondary, line_valid, first_valid, last_valid, az_coef, az_base, rg_base, rg_coef, block_dest
):
    cols = secondary.shape[2]
    blocks = block_dest.shape[0]
    tiles = cols // 128
    count = lax.axis_size("az")
    col = jnp.arange(cols, dtype=jnp.int32)
    kept = (
        (line_valid[:, None] > 0)
        & (col[None, :] >= first_valid[:, None])
        & (col[None, :] < last_valid[:, None])
    )
    masked = jnp.where(kept[None], secondary, jnp.zeros((), jnp.bfloat16))
    forward = [(i, i + 1) for i in range(count - 1)]
    backward = [(b, a) for a, b in forward]
    low = lax.ppermute(masked[:, blocks - HALO :], "az", forward)
    high = lax.ppermute(masked[:, :HALO], "az", backward)
    band = azimuth_band(az_coef, az_base)
    smem = pl.BlockSpec(memory_space=pltpu.SMEM)
    vmem = pl.BlockSpec(memory_space=pltpu.VMEM)
    sent = pl.pallas_call(
        filter_kernel,
        out_shape=jax.ShapeDtypeStruct((blocks, 2 * tiles + META, 128), jnp.bfloat16),
        in_specs=[smem] * 6 + [vmem] * 4,
        out_specs=vmem,
        scratch_shapes=[
            pltpu.VMEM((2 * blocks * (tiles + 2 * PAD), 128), jnp.float32),
            pltpu.VMEM((tiles // 8, TAPS, 8, 128), jnp.float32),
            pltpu.SMEM((tiles // 8,), jnp.int32),
        ],
        cost_estimate=pl.CostEstimate(
            flops=40 * 2 * blocks * cols, bytes_accessed=8 * blocks * cols, transcendentals=0
        ),
        name="filters",
    )(rg_coef, rg_base, block_dest, line_valid, first_valid, last_valid, band, masked, low, high)
    got = lax.all_to_all(sent, "az", split_axis=0, concat_axis=0, tiled=True)
    return pl.pallas_call(
        functools.partial(finish_kernel, cols * blocks * count),
        out_shape=(
            jax.ShapeDtypeStruct((2, blocks, cols), jnp.bfloat16),
            jax.ShapeDtypeStruct((1,), jnp.float32),
            jax.ShapeDtypeStruct((1,), jnp.float32),
        ),
        in_specs=[vmem],
        out_specs=(vmem, smem, smem),
        scratch_shapes=[pltpu.VMEM((2 * blocks * tiles, 128), jnp.float32)],
        name="finish",
    )(got)


def solution(mesh):
    rows = P(("scene", "az"))
    placed = (
        P(None, ("scene", "az"), None),
        rows,
        rows,
        rows,
        P(None, ("scene", "az")),
        rows,
        rows,
        P("scene"),
        rows,
    )
    return jax.shard_map(
        shards,
        mesh=mesh,
        in_specs=placed,
        out_specs=(P(None, ("scene", "az"), None), P("scene"), P("scene")),
        check_vma=False,
    )
```

```python
import functools

import jax
import jax.numpy as jnp
from jax import lax
from jax.experimental import pallas as pl
from jax.experimental.pallas import tpu as pltpu
from jax.sharding import PartitionSpec as P

HALO = 8
TAPS = 11
NOTE = 8
STEP = 512
PI = 3.141592653589793
HALF = 0.7071067811865476
COS8 = (1.0, HALF, 0.0, -HALF, -1.0, -HALF, 0.0, HALF)


def range_weights(coef, start, weight, cols):
    for g in range(cols // 1024):
        centre = (g * 1024 + 512) / cols
        oc = coef[0] + coef[1] * centre + coef[2] * (centre * centre) + coef[3] * (centre**3)
        n0 = (oc - 5.0 + 64.0).astype(jnp.int32) - 63
        start[g] = n0
        sub = lax.broadcasted_iota(jnp.int32, (8, 128), 0)
        lane = lax.broadcasted_iota(jnp.int32, (8, 128), 1)
        col = g * 1024 + sub * 128 + lane
        v = (col.astype(jnp.float32) + 0.5) / cols
        off = coef[0] + coef[1] * v + coef[2] * v * v + coef[3] * v * v * v
        whole = jnp.round(off)
        part = off - whole
        odd = (whole.astype(jnp.int32) + n0) & 1
        sine = jnp.sin(PI * part) * (-1.0 / PI) * (1 - 2 * odd).astype(jnp.float32)
        base = (n0.astype(jnp.float32) - off) * (PI / 4.0)
        c0, s0 = jnp.cos(base), jnp.sin(base)
        for k in range(TAPS):
            n = n0 + k
            d = n.astype(jnp.float32) - off
            ck, sk = COS8[k % 8], COS8[(k - 2) % 8]
            taper = 0.5 + 0.5 * (c0 * ck - s0 * sk)
            top = sine if k % 2 == 0 else -sine
            near = d == 0.0
            val = jnp.where(near, 1.0, top / jnp.where(near, 1.0, d)) * taper
            keep = (jnp.abs(d) < 4.0) & (col + n >= 0) & (col + n < cols)
            val = jnp.where(keep, val, 0.0)
            weight[g, k] = val.astype(jnp.bfloat16).astype(jnp.float32)


def column(values):
    row = lax.broadcasted_iota(jnp.int32, (len(values), 128), 0)
    made = jnp.zeros((len(values), 128), jnp.asarray(values[0]).dtype)
    for r, value in enumerate(values):
        made = jnp.where(row == r, value, made)
    return made


def azimuth_band(fraction, base, line, blocks):
    held = lax.broadcasted_iota(jnp.int32, (blocks, 128), 1)
    row = jnp.where(held < blocks, held, held - blocks - HALO)
    row = jnp.where(held < blocks + HALO, row, held - HALO)
    gap = row - line - base
    d = gap.astype(jnp.float32) - fraction
    near = d == 0.0
    safe = jnp.where(near, 1.0, d)
    whole = jnp.round(safe)
    sine = jnp.sin(PI * (safe - whole)) * (1 - 2 * (whole.astype(jnp.int32) & 1)).astype(jnp.float32)
    value = jnp.where(near, 1.0, sine / (PI * safe)) * (0.5 + 0.5 * jnp.cos(PI * d / 4.0))
    keep = (jnp.abs(d) < 4.0) & (jnp.abs(gap) <= 4) & (held < blocks + 2 * HALO)
    return jnp.where(keep, value, 0.0).astype(jnp.bfloat16)


def swath_kernel(
    chunks, coef, shift, dest, valid, first, last, az_coef, az_base, image,
    got, notes,
    held, edge, dense, weight, sent, memo, start, order,
    own_sem, halo_send, halo_recv, edge_send, edge_recv, send_sem, recv_sem, note_send, note_recv,
):
    blocks, cols = image.shape[1], image.shape[2]
    tiles = cols // 128
    span = dense.shape[0] // (2 * blocks)
    count = lax.axis_size("az")
    me = lax.axis_index("az")
    after, before = lax.rem(me + 1, count), lax.rem(me + count - 1, count)
    own = pltpu.make_async_copy(image, held.at[:, pl.ds(0, blocks)], own_sem)
    own.start()

    barrier = pltpu.get_barrier_semaphore()

    def greet(i, carry):
        pl.semaphore_signal(barrier, inc=1, device_id={"az": lax.rem(me + 1 + i, count)})
        return carry

    lax.fori_loop(0, count - 1, greet, 0)
    low_edge = [jnp.where(valid[r] > 0, first[r], cols) for r in range(blocks)]
    high_edge = [jnp.where(valid[r] > 0, last[r], 0) for r in range(blocks)]
    edge[0, pl.ds(0, blocks), :] = column(low_edge).astype(jnp.float32)
    edge[1, pl.ds(0, blocks), :] = column(high_edge).astype(jnp.float32)
    pl.semaphore_wait(barrier, count - 1)

    steps = cols // STEP
    bounds = [0] + [steps * (c + 1) // chunks + 1 for c in range(chunks - 1)] + [steps]
    ways = ((after, blocks - HALO, blocks), (before, 0, blocks + HALO))
    for w, (peer, source, slot) in enumerate(ways):
        pltpu.make_async_remote_copy(
            src_ref=edge.at[:, pl.ds(source, HALO), :],
            dst_ref=edge.at[:, pl.ds(slot, HALO), :],
            send_sem=edge_send.at[w],
            recv_sem=edge_recv.at[w],
            device_id={"az": peer},
        ).start()
    halo = []
    for c in range(chunks):
        at = pl.ds(bounds[c] * STEP, (bounds[c + 1] - bounds[c]) * STEP)
        for w, (peer, source, slot) in enumerate(ways):
            copy = pltpu.make_async_remote_copy(
                src_ref=image.at[:, pl.ds(source, HALO), at],
                dst_ref=held.at[:, pl.ds(slot, HALO), at],
                send_sem=halo_send.at[c, w],
                recv_sem=halo_recv.at[c, w],
                device_id={"az": peer},
            )
            copy.start()
            halo.append(copy)

    range_weights(coef, start, weight, cols)
    lines = []
    for i in range(blocks):
        target = lax.rem(me + 1 + i, count)
        line = jnp.int32(0)
        for j in range(blocks):
            line = jnp.where(dest[j] // blocks == target, j, line)
        order[i] = line
        lines.append(line)
    c0 = column([az_coef[0, j] for j in lines])
    c1 = column([az_coef[1, j] for j in lines])
    c2 = column([az_coef[2, j] for j in lines])
    q = 0.5
    fraction = c0 + c1 * q + c2 * q * q
    band = azimuth_band(fraction, column([az_base[j] for j in lines]), column(lines), blocks)
    band = band[:, : blocks + 2 * HALO]

    own.wait()
    for w, (peer, source, slot) in enumerate(ways):
        pltpu.make_async_remote_copy(
            src_ref=edge.at[:, pl.ds(source, HALO), :],
            dst_ref=edge.at[:, pl.ds(slot, HALO), :],
            send_sem=edge_send.at[w],
            recv_sem=edge_recv.at[w],
            device_id={"az": peer},
        ).wait()
    low = edge[0]
    high = edge[1]
    row = lax.broadcasted_iota(jnp.int32, high.shape, 0)
    outside = ((me == 0) & (row >= blocks) & (row < blocks + HALO)) | (
        (me == count - 1) & (row >= blocks + HALO)
    )
    high = jnp.where(outside, 0.0, high)
    lane_held = lax.broadcasted_iota(jnp.int32, high.shape, 1).astype(jnp.float32)
    lane_row = lax.broadcasted_iota(jnp.int32, (blocks, 128), 1)
    lane = lax.broadcasted_iota(jnp.int32, (8, 128), 1)

    def azimuth(s, tails):
        at = pl.ds(pl.multiple_of(s * STEP, STEP), STEP)
        keeps = []
        for u in range(STEP // 128):
            col = lane_held + (s * STEP + u * 128).astype(jnp.float32)
            keeps.append((col >= low) & (col < high))
        new_tails = []
        for p in range(2):
            rows = held[p, :, at].astype(jnp.float32)
            rows = jnp.concatenate(
                [
                    jnp.where(keep, rows[:, u * 128 : u * 128 + 128], 0.0)
                    for u, keep in enumerate(keeps)
                ],
                axis=1,
            ).astype(jnp.bfloat16)
            out = jnp.dot(band, rows, preferred_element_type=jnp.float32)
            out = out.astype(jnp.bfloat16).astype(jnp.float32)
            tail = tails[p]
            for u in range(STEP // 128):
                turned = pltpu.roll(out[:, u * 128 : u * 128 + 128], 64, 1)
                place = p * blocks * span + s * (STEP // 128) + u
                dense[pl.ds(place, blocks, stride=span), :] = jnp.where(lane_row < 64, tail, turned)
                tail = turned
            new_tails.append(tail)
        return tuple(new_tails)

    def filtered(i, big, power):
        for p in range(2):
            halves = []
            for h in range(2):
                g = big * 2 + h
                b = shift[order[i]] + start[g] + 64
                at = pl.multiple_of((p * blocks + i) * span + g * 8, 8)
                x0 = dense[pl.ds(at, 8), :]
                x1 = dense[pl.ds(at + 1, 8), :]
                acc = None
                for k in range(TAPS):
                    moved = pltpu.roll(jnp.where(lane < b + k, x1, x0), 128 - b - k, 1)
                    term = weight[g, k] * moved
                    acc = term if acc is None else acc + term
                halves.append(acc)
            done = jnp.concatenate(halves, axis=0).astype(jnp.bfloat16)
            sent[i, p, pl.ds(pl.multiple_of(big * 16, 16), 16), :] = done
            wide = done.astype(jnp.float32)
            power = power + wide * wide
        return power

    tails = (jnp.zeros((blocks, 128), jnp.float32),) * 2
    power = jnp.zeros((16, 128), jnp.float32)
    bigs = tiles // 16
    for c in range(chunks):
        for copy in halo[2 * c : 2 * c + 2]:
            copy.wait()
        tails = lax.fori_loop(bounds[c], bounds[c + 1], azimuth, tails)
        if c == chunks - 1:
            for p in range(2):
                ends = jnp.where(lane_row < 64, tails[p], 0.0)
                dense[pl.ds(p * blocks * span + tiles, blocks, stride=span), :] = ends
        lo, hi = bigs * c // chunks, bigs * (c + 1) // chunks
        at = pl.ds(lo * 16, (hi - lo) * 16)

        def line(i, power):
            power = lax.fori_loop(lo, hi, functools.partial(filtered, i), power, unroll=True)

            @pl.when(i < count - 1)
            def _():
                pltpu.make_async_remote_copy(
                    src_ref=sent.at[i, :, at, :],
                    dst_ref=got.at[me, :, at, :],
                    send_sem=send_sem.at[c, i],
                    recv_sem=recv_sem.at[c, me],
                    device_id={"az": lax.rem(me + 1 + i, count)},
                ).start()

            return power

        power = lax.fori_loop(0, blocks, line, power)

    own_power = jnp.broadcast_to(jnp.sum(power, keepdims=True), (NOTE, 128))
    have = jnp.int32(0)
    for j in range(blocks):
        have = have + jnp.maximum(
            jnp.minimum(high_edge[j], cols) - jnp.maximum(low_edge[j], 0), 0
        )
    own_count = jnp.full((NOTE, 128), have, jnp.int32).astype(jnp.float32)
    row = lax.broadcasted_iota(jnp.int32, (NOTE, 128), 0)
    stats = jnp.where(row == 1, own_power, own_count)
    for i in range(blocks):
        place = jnp.full((NOTE, 128), dest[lines[i]] % blocks, jnp.int32).astype(jnp.float32)
        memo[i] = jnp.where(row == 0, place, stats)

    def tell(i, carry):
        pltpu.make_async_remote_copy(
            src_ref=memo.at[i],
            dst_ref=notes.at[me],
            send_sem=note_send.at[i],
            recv_sem=note_recv.at[me],
            device_id={"az": lax.rem(me + 1 + i, count)},
        ).start()
        return carry

    lax.fori_loop(0, count - 1, tell, 0)
    notes[me] = memo[blocks - 1]
    got[me] = sent[blocks - 1]

    def take(i, carry):
        peer = lax.rem(me + 1 + i, count)
        for c in range(chunks):
            lo, hi = bigs * c // chunks, bigs * (c + 1) // chunks
            at = pl.ds(lo * 16, (hi - lo) * 16)
            done = pltpu.make_async_remote_copy(
                src_ref=sent.at[i, :, at, :],
                dst_ref=got.at[peer, :, at, :],
                send_sem=send_sem.at[c, i],
                recv_sem=recv_sem.at[c, peer],
                device_id={"az": peer},
            )
            done.wait_send()
            done.wait_recv()
        told = pltpu.make_async_remote_copy(
            src_ref=memo.at[i],
            dst_ref=notes.at[peer],
            send_sem=note_send.at[i],
            recv_sem=note_recv.at[peer],
            device_id={"az": peer},
        )
        told.wait_send()
        told.wait_recv()
        return carry

    lax.fori_loop(0, count - 1, take, 0)


def finish_kernel(total, got, notes, out, mean, share, wide):
    blocks, cols = out.shape[1], out.shape[2]
    tiles = cols // 128
    told = [notes[s] for s in range(blocks)]
    both = functools.reduce(lambda a, b: a + b, told)
    power, count = both[1:2], both[2:3]
    mean_power = power / jnp.maximum(count, 1.0)
    gain = lax.rsqrt(mean_power + 0.5)
    mean[0] = mean_power[0, 0]
    share[0] = (count / float(total))[0, 0]
    for s in range(blocks):
        place = told[s][0, 0].astype(jnp.int32)
        for p in range(2):
            x = got[s, p].astype(jnp.float32) * gain
            wide[pl.ds(pl.multiple_of((p * blocks + place) * tiles, 8), tiles), :] = x

    def tile(t, carry):
        at = pl.ds(pl.multiple_of(t * 128, 128), 128)
        for p in range(2):
            x = wide[pl.ds(p * blocks * tiles + t, blocks, stride=tiles), :]
            out[p, :, at] = x.astype(jnp.bfloat16)
        return carry

    lax.fori_loop(0, tiles, tile, 0, unroll=8)


def shards(
    secondary, line_valid, first_valid, last_valid, az_coef, az_base, rg_base, rg_coef, block_dest
):
    cols = secondary.shape[2]
    blocks = block_dest.shape[0]
    tiles = cols // 128
    count = lax.axis_size("az")
    bigs = tiles // 16
    chunks = max(c for c in range(1, CHUNKS + 1) if bigs % c == 0)
    smem = pl.BlockSpec(memory_space=pltpu.SMEM)
    vmem = pl.BlockSpec(memory_space=pltpu.VMEM)
    held = blocks + 2 * HALO
    dma = pltpu.SemaphoreType.DMA
    got, notes = pl.pallas_call(
        functools.partial(swath_kernel, chunks),
        out_shape=(
            jax.ShapeDtypeStruct((blocks, 2, tiles, 128), jnp.bfloat16),
            jax.ShapeDtypeStruct((blocks, NOTE, 128), jnp.float32),
        ),
        in_specs=[smem] * 8 + [pl.BlockSpec(memory_space=pl.ANY)],
        out_specs=(vmem, vmem),
        scratch_shapes=[
            pltpu.VMEM((2, held, cols), jnp.bfloat16),
            pltpu.VMEM((2, held, 128), jnp.float32),
            pltpu.VMEM((2 * blocks * (tiles + 8), 128), jnp.float32),
            pltpu.VMEM((tiles // 8, TAPS, 8, 128), jnp.float32),
            pltpu.VMEM((blocks, 2, tiles, 128), jnp.bfloat16),
            pltpu.VMEM((blocks, NOTE, 128), jnp.float32),
            pltpu.SMEM((tiles // 8,), jnp.int32),
            pltpu.SMEM((blocks,), jnp.int32),
            dma(()),
            dma((chunks, 2)),
            dma((chunks, 2)),
            dma((2,)),
            dma((2,)),
            dma((chunks, blocks)),
            dma((chunks, blocks)),
            dma((blocks,)),
            dma((blocks,)),
        ],
        compiler_params=pltpu.CompilerParams(collective_id=0, has_side_effects=True),
        name="swath",
    )(
        rg_coef, rg_base, block_dest, line_valid, first_valid, last_valid, az_coef, az_base,
        secondary,
    )
    return pl.pallas_call(
        functools.partial(finish_kernel, cols * blocks * count),
        out_shape=(
            jax.ShapeDtypeStruct((2, blocks, cols), jnp.bfloat16),
            jax.ShapeDtypeStruct((1,), jnp.float32),
            jax.ShapeDtypeStruct((1,), jnp.float32),
        ),
        in_specs=[vmem, vmem],
        out_specs=(vmem, smem, smem),
        scratch_shapes=[pltpu.VMEM((2 * blocks * tiles, 128), jnp.float32)],
        name="finish",
    )(got, notes)


CHUNKS = 3


def solution(mesh):
    rows = P(("scene", "az"))
    placed = (
        P(None, ("scene", "az"), None),
        rows,
        rows,
        rows,
        P(None, ("scene", "az")),
        rows,
        rows,
        P("scene"),
        rows,
    )
    return jax.shard_map(
        shards,
        mesh=mesh,
        in_specs=placed,
        out_specs=(P(None, ("scene", "az"), None), P("scene"), P("scene")),
        check_vma=False,
    )
```

```python
import functools

import jax
import jax.numpy as jnp
from jax import lax
from jax.experimental import pallas as pl
from jax.experimental.pallas import tpu as pltpu
from jax.sharding import PartitionSpec as P

HALO = 8
TAPS = 11
NOTE = 8
STEP = 512
PI = 3.141592653589793
HALF = 0.7071067811865476
COS8 = (1.0, HALF, 0.0, -HALF, -1.0, -HALF, 0.0, HALF)


def range_weights(coef, start, weight, cols):
    for g in range(cols // 1024):
        centre = (g * 1024 + 512) / cols
        oc = coef[0] + coef[1] * centre + coef[2] * (centre * centre) + coef[3] * (centre**3)
        n0 = (oc - 5.0 + 64.0).astype(jnp.int32) - 63
        start[g] = n0
        sub = lax.broadcasted_iota(jnp.int32, (8, 128), 0)
        lane = lax.broadcasted_iota(jnp.int32, (8, 128), 1)
        col = g * 1024 + sub * 128 + lane
        v = (col.astype(jnp.float32) + 0.5) / cols
        off = coef[0] + coef[1] * v + coef[2] * v * v + coef[3] * v * v * v
        whole = jnp.round(off)
        part = off - whole
        odd = (whole.astype(jnp.int32) + n0) & 1
        sine = jnp.sin(PI * part) * (-1.0 / PI) * (1 - 2 * odd).astype(jnp.float32)
        base = (n0.astype(jnp.float32) - off) * (PI / 4.0)
        c0, s0 = jnp.cos(base), jnp.sin(base)
        for k in range(TAPS):
            n = n0 + k
            d = n.astype(jnp.float32) - off
            ck, sk = COS8[k % 8], COS8[(k - 2) % 8]
            taper = 0.5 + 0.5 * (c0 * ck - s0 * sk)
            top = sine if k % 2 == 0 else -sine
            near = d == 0.0
            val = jnp.where(near, 1.0, top / jnp.where(near, 1.0, d)) * taper
            keep = (jnp.abs(d) < 4.0) & (col + n >= 0) & (col + n < cols)
            val = jnp.where(keep, val, 0.0)
            weight[g, k] = val.astype(jnp.bfloat16).astype(jnp.float32)


def column(values):
    row = lax.broadcasted_iota(jnp.int32, (len(values), 128), 0)
    made = jnp.zeros((len(values), 128), jnp.asarray(values[0]).dtype)
    for r, value in enumerate(values):
        made = jnp.where(row == r, value, made)
    return made


def azimuth_band(fraction, base, line, blocks):
    held = lax.broadcasted_iota(jnp.int32, (blocks, 128), 1)
    row = jnp.where(held < blocks, held, held - blocks - HALO)
    row = jnp.where(held < blocks + HALO, row, held - HALO)
    gap = row - line - base
    d = gap.astype(jnp.float32) - fraction
    near = d == 0.0
    safe = jnp.where(near, 1.0, d)
    whole = jnp.round(safe)
    sine = jnp.sin(PI * (safe - whole)) * (1 - 2 * (whole.astype(jnp.int32) & 1)).astype(jnp.float32)
    value = jnp.where(near, 1.0, sine / (PI * safe)) * (0.5 + 0.5 * jnp.cos(PI * d / 4.0))
    keep = (jnp.abs(d) < 4.0) & (jnp.abs(gap) <= 4) & (held < blocks + 2 * HALO)
    return jnp.where(keep, value, 0.0).astype(jnp.bfloat16)


def send_order(me, count, i):
    half = count // 2
    mine = me // half
    own = i // half
    side = mine * own + (1 - mine) * (1 - own)
    return side * half + lax.rem(me - mine * half + own + i - own * half, half)


def swath_kernel(
    cuts, coef, shift, dest, valid, first, last, az_coef, az_base, image,
    got, notes,
    held, edge, dense, weight, sent, memo, start, order,
    own_sem, halo_send, halo_recv, edge_send, edge_recv, send_sem, recv_sem, note_send, note_recv,
):
    blocks, cols = image.shape[1], image.shape[2]
    tiles = cols // 128
    span = dense.shape[0] // (2 * blocks)
    count = lax.axis_size("az")
    me = lax.axis_index("az")
    after, before = lax.rem(me + 1, count), lax.rem(me + count - 1, count)
    own = pltpu.make_async_copy(image, held.at[:, pl.ds(0, blocks)], own_sem)
    own.start()

    barrier = pltpu.get_barrier_semaphore()

    def greet(i, carry):
        pl.semaphore_signal(barrier, inc=1, device_id={"az": lax.rem(me + 1 + i, count)})
        return carry

    lax.fori_loop(0, count - 1, greet, 0)
    low_edge = [jnp.where(valid[r] > 0, first[r], cols) for r in range(blocks)]
    high_edge = [jnp.where(valid[r] > 0, last[r], 0) for r in range(blocks)]
    edge[0, pl.ds(0, blocks), :] = column(low_edge).astype(jnp.float32)
    edge[1, pl.ds(0, blocks), :] = column(high_edge).astype(jnp.float32)
    range_weights(coef, start, weight, cols)
    lines = []
    for i in range(blocks):
        target = send_order(me, count, i)
        line = jnp.int32(0)
        for j in range(blocks):
            line = jnp.where(dest[j] // blocks == target, j, line)
        order[i] = line
        lines.append(line)
    c0 = column([az_coef[0, j] for j in lines])
    c1 = column([az_coef[1, j] for j in lines])
    c2 = column([az_coef[2, j] for j in lines])
    q = 0.5
    fraction = c0 + c1 * q + c2 * q * q
    band = azimuth_band(fraction, column([az_base[j] for j in lines]), column(lines), blocks)
    band = band[:, : blocks + 2 * HALO]

    pl.semaphore_wait(barrier, count - 1)

    steps = cols // STEP
    chunks = len(cuts) - 1
    per = steps // (tiles // 16)
    bounds = [0] + [cut * per + 1 for cut in cuts[1:-1]] + [steps]
    ways = ((after, blocks - HALO, blocks), (before, 0, blocks + HALO))
    for w, (peer, source, slot) in enumerate(ways):
        pltpu.make_async_remote_copy(
            src_ref=edge.at[:, pl.ds(source, HALO), :],
            dst_ref=edge.at[:, pl.ds(slot, HALO), :],
            send_sem=edge_send.at[w],
            recv_sem=edge_recv.at[w],
            device_id={"az": peer},
        ).start()
    halo = []
    for c in range(chunks):
        at = pl.ds(bounds[c] * STEP, (bounds[c + 1] - bounds[c]) * STEP)
        for w, (peer, source, slot) in enumerate(ways):
            copy = pltpu.make_async_remote_copy(
                src_ref=image.at[:, pl.ds(source, HALO), at],
                dst_ref=held.at[:, pl.ds(slot, HALO), at],
                send_sem=halo_send.at[c, w],
                recv_sem=halo_recv.at[c, w],
                device_id={"az": peer},
            )
            copy.start()
            halo.append(copy)

    own.wait()
    for w, (peer, source, slot) in enumerate(ways):
        pltpu.make_async_remote_copy(
            src_ref=edge.at[:, pl.ds(source, HALO), :],
            dst_ref=edge.at[:, pl.ds(slot, HALO), :],
            send_sem=edge_send.at[w],
            recv_sem=edge_recv.at[w],
            device_id={"az": peer},
        ).wait()
    low = edge[0]
    high = edge[1]
    row = lax.broadcasted_iota(jnp.int32, high.shape, 0)
    outside = ((me == 0) & (row >= blocks) & (row < blocks + HALO)) | (
        (me == count - 1) & (row >= blocks + HALO)
    )
    high = jnp.where(outside, 0.0, high)
    lane_held = lax.broadcasted_iota(jnp.int32, high.shape, 1).astype(jnp.float32)
    lane_row = lax.broadcasted_iota(jnp.int32, (blocks, 128), 1)
    lane = lax.broadcasted_iota(jnp.int32, (8, 128), 1)

    def azimuth(s, tails):
        at = pl.ds(pl.multiple_of(s * STEP, STEP), STEP)
        keeps = []
        for u in range(STEP // 128):
            col = lane_held + (s * STEP + u * 128).astype(jnp.float32)
            keeps.append((col >= low) & (col < high))
        new_tails = []
        for p in range(2):
            rows = held[p, :, at].astype(jnp.float32)
            rows = jnp.concatenate(
                [
                    jnp.where(keep, rows[:, u * 128 : u * 128 + 128], 0.0)
                    for u, keep in enumerate(keeps)
                ],
                axis=1,
            ).astype(jnp.bfloat16)
            out = jnp.dot(band, rows, preferred_element_type=jnp.float32)
            out = out.astype(jnp.bfloat16).astype(jnp.float32)
            tail = tails[p]
            for u in range(STEP // 128):
                turned = pltpu.roll(out[:, u * 128 : u * 128 + 128], 64, 1)
                place = p * blocks * span + s * (STEP // 128) + u
                dense[pl.ds(place, blocks, stride=span), :] = jnp.where(lane_row < 64, tail, turned)
                tail = turned
            new_tails.append(tail)
        return tuple(new_tails)

    def filtered(i, big, power):
        for p in range(2):
            halves = []
            for h in range(2):
                g = big * 2 + h
                b = shift[order[i]] + start[g] + 64
                at = pl.multiple_of((p * blocks + i) * span + g * 8, 8)
                x0 = dense[pl.ds(at, 8), :]
                x1 = dense[pl.ds(at + 1, 8), :]
                acc = None
                for k in range(TAPS):
                    moved = pltpu.roll(jnp.where(lane < b + k, x1, x0), 128 - b - k, 1)
                    term = weight[g, k] * moved
                    acc = term if acc is None else acc + term
                halves.append(acc)
            done = jnp.concatenate(halves, axis=0).astype(jnp.bfloat16)
            sent[i, p, pl.ds(pl.multiple_of(big * 16, 16), 16), :] = done
            wide = done.astype(jnp.float32)
            power = power + wide * wide
        return power

    tails = (jnp.zeros((blocks, 128), jnp.float32),) * 2
    power = jnp.zeros((16, 128), jnp.float32)
    for c in range(chunks):
        for copy in halo[2 * c : 2 * c + 2]:
            copy.wait()
        tails = lax.fori_loop(bounds[c], bounds[c + 1], azimuth, tails)
        if c == chunks - 1:
            for p in range(2):
                ends = jnp.where(lane_row < 64, tails[p], 0.0)
                dense[pl.ds(p * blocks * span + tiles, blocks, stride=span), :] = ends
        lo, hi = cuts[c], cuts[c + 1]
        at = pl.ds(lo * 16, (hi - lo) * 16)

        def line(i, power):
            power = lax.fori_loop(lo, hi, functools.partial(filtered, i), power, unroll=True)

            @pl.when(i < count - 1)
            def _():
                pltpu.make_async_remote_copy(
                    src_ref=sent.at[i, :, at, :],
                    dst_ref=got.at[me, :, at, :],
                    send_sem=send_sem.at[c, i],
                    recv_sem=recv_sem.at[c, me],
                    device_id={"az": send_order(me, count, i)},
                ).start()

            return power

        power = lax.fori_loop(0, blocks, line, power)

    own_power = jnp.broadcast_to(jnp.sum(power, keepdims=True), (NOTE, 128))
    have = jnp.int32(0)
    for j in range(blocks):
        have = have + jnp.maximum(
            jnp.minimum(high_edge[j], cols) - jnp.maximum(low_edge[j], 0), 0
        )
    own_count = jnp.full((NOTE, 128), have, jnp.int32).astype(jnp.float32)
    row = lax.broadcasted_iota(jnp.int32, (NOTE, 128), 0)
    stats = jnp.where(row == 1, own_power, own_count)
    for i in range(blocks):
        place = jnp.full((NOTE, 128), dest[lines[i]] % blocks, jnp.int32).astype(jnp.float32)
        memo[i] = jnp.where(row == 0, place, stats)

    def tell(i, carry):
        pltpu.make_async_remote_copy(
            src_ref=memo.at[i],
            dst_ref=notes.at[me],
            send_sem=note_send.at[i],
            recv_sem=note_recv.at[me],
            device_id={"az": send_order(me, count, i)},
        ).start()
        return carry

    lax.fori_loop(0, count - 1, tell, 0)
    notes[me] = memo[blocks - 1]
    got[me] = sent[blocks - 1]

    def take(i, carry):
        peer = send_order(me, count, i)
        for c in range(chunks):
            lo, hi = cuts[c], cuts[c + 1]
            at = pl.ds(lo * 16, (hi - lo) * 16)
            done = pltpu.make_async_remote_copy(
                src_ref=sent.at[i, :, at, :],
                dst_ref=got.at[peer, :, at, :],
                send_sem=send_sem.at[c, i],
                recv_sem=recv_sem.at[c, peer],
                device_id={"az": peer},
            )
            done.wait_send()
            done.wait_recv()
        told = pltpu.make_async_remote_copy(
            src_ref=memo.at[i],
            dst_ref=notes.at[peer],
            send_sem=note_send.at[i],
            recv_sem=note_recv.at[peer],
            device_id={"az": peer},
        )
        told.wait_send()
        told.wait_recv()
        return carry

    lax.fori_loop(0, count - 1, take, 0)


def finish_kernel(total, got, notes, out, mean, share, wide):
    blocks, cols = out.shape[1], out.shape[2]
    tiles = cols // 128
    told = [notes[s] for s in range(blocks)]
    both = functools.reduce(lambda a, b: a + b, told)
    power, count = both[1:2], both[2:3]
    mean_power = power / jnp.maximum(count, 1.0)
    gain = lax.rsqrt(mean_power + 0.5)
    mean[0] = mean_power[0, 0]
    share[0] = (count / float(total))[0, 0]
    for s in range(blocks):
        place = told[s][0, 0].astype(jnp.int32)
        for p in range(2):
            x = got[s, p].astype(jnp.float32) * gain
            wide[pl.ds(pl.multiple_of((p * blocks + place) * tiles, 8), tiles), :] = x
    for t in range(tiles):
        for p in range(2):
            x = wide[pl.ds(p * blocks * tiles + t, blocks, stride=tiles), :]
            out[p, :, t * 128 : t * 128 + 128] = x.astype(jnp.bfloat16)


def shards(
    secondary, line_valid, first_valid, last_valid, az_coef, az_base, rg_base, rg_coef, block_dest
):
    cols = secondary.shape[2]
    blocks = block_dest.shape[0]
    tiles = cols // 128
    count = lax.axis_size("az")
    bigs = tiles // 16
    cuts = [0] + sorted({bigs * cut // 6 for cut in CUTS} - {0, bigs}) + [bigs]
    chunks = len(cuts) - 1
    parts = max(c for c in range(1, PARTS + 1) if bigs % c == 0)
    smem = pl.BlockSpec(memory_space=pltpu.SMEM)
    vmem = pl.BlockSpec(memory_space=pltpu.VMEM)
    held = blocks + 2 * HALO
    dma = pltpu.SemaphoreType.DMA
    got, notes = pl.pallas_call(
        functools.partial(swath_kernel, cuts),
        out_shape=(
            jax.ShapeDtypeStruct((blocks, 2, tiles, 128), jnp.bfloat16),
            jax.ShapeDtypeStruct((blocks, NOTE, 128), jnp.float32),
        ),
        in_specs=[smem] * 8 + [pl.BlockSpec(memory_space=pl.ANY)],
        out_specs=(vmem, vmem),
        scratch_shapes=[
            pltpu.VMEM((2, held, cols), jnp.bfloat16),
            pltpu.VMEM((2, held, 128), jnp.float32),
            pltpu.VMEM((2 * blocks * (tiles + 8), 128), jnp.float32),
            pltpu.VMEM((tiles // 8, TAPS, 8, 128), jnp.float32),
            pltpu.VMEM((blocks, 2, tiles, 128), jnp.bfloat16),
            pltpu.VMEM((blocks, NOTE, 128), jnp.float32),
            pltpu.SMEM((tiles // 8,), jnp.int32),
            pltpu.SMEM((blocks,), jnp.int32),
            dma(()),
            dma((chunks, 2)),
            dma((chunks, 2)),
            dma((2,)),
            dma((2,)),
            dma((chunks, blocks)),
            dma((chunks, blocks)),
            dma((blocks,)),
            dma((blocks,)),
        ],
        compiler_params=pltpu.CompilerParams(collective_id=0, has_side_effects=True),
        name="swath",
    )(
        rg_coef, rg_base, block_dest, line_valid, first_valid, last_valid, az_coef, az_base,
        secondary,
    )
    return pl.pallas_call(
        functools.partial(finish_kernel, cols * blocks * count),
        out_shape=(
            jax.ShapeDtypeStruct((2, blocks, cols), jnp.bfloat16),
            jax.ShapeDtypeStruct((1,), jnp.float32),
            jax.ShapeDtypeStruct((1,), jnp.float32),
        ),
        grid=(parts,),
        in_specs=[pl.BlockSpec((blocks, 2, tiles // parts, 128), lambda c: (0, 0, c, 0)), vmem],
        out_specs=(pl.BlockSpec((2, blocks, cols // parts), lambda c: (0, 0, c)), smem, smem),
        scratch_shapes=[pltpu.VMEM((2 * blocks * (tiles // parts), 128), jnp.float32)],
        name="finish",
    )(got, notes)


CUTS = (2,)
PARTS = 2


def solution(mesh):
    rows = P(("scene", "az"))
    placed = (
        P(None, ("scene", "az"), None),
        rows,
        rows,
        rows,
        P(None, ("scene", "az")),
        rows,
        rows,
        P("scene"),
        rows,
    )
    return jax.shard_map(
        shards,
        mesh=mesh,
        in_specs=placed,
        out_specs=(P(None, ("scene", "az"), None), P("scene"), P("scene")),
        check_vma=False,
    )
```

```python
import functools

import jax
import jax.numpy as jnp
from jax import lax
from jax.experimental import pallas as pl
from jax.experimental.pallas import tpu as pltpu
from jax.sharding import PartitionSpec as P

HALO = 8
TAPS = 11
NOTE = 8
STEP = 512
PI = 3.141592653589793
HALF = 0.7071067811865476
COS8 = (1.0, HALF, 0.0, -HALF, -1.0, -HALF, 0.0, HALF)


def range_weights(coef, start, weight, cols):
    for g in range(cols // 1024):
        centre = (g * 1024 + 512) / cols
        oc = coef[0] + coef[1] * centre + coef[2] * (centre * centre) + coef[3] * (centre**3)
        n0 = (oc - 5.0 + 64.0).astype(jnp.int32) - 63
        start[g] = n0
        sub = lax.broadcasted_iota(jnp.int32, (8, 128), 0)
        lane = lax.broadcasted_iota(jnp.int32, (8, 128), 1)
        col = g * 1024 + sub * 128 + lane
        v = (col.astype(jnp.float32) + 0.5) / cols
        off = coef[0] + coef[1] * v + coef[2] * v * v + coef[3] * v * v * v
        whole = jnp.round(off)
        part = off - whole
        odd = (whole.astype(jnp.int32) + n0) & 1
        sine = jnp.sin(PI * part) * (-1.0 / PI) * (1 - 2 * odd).astype(jnp.float32)
        base = (n0.astype(jnp.float32) - off) * (PI / 4.0)
        c0, s0 = jnp.cos(base), jnp.sin(base)
        for k in range(TAPS):
            n = n0 + k
            d = n.astype(jnp.float32) - off
            ck, sk = COS8[k % 8], COS8[(k - 2) % 8]
            taper = 0.5 + 0.5 * (c0 * ck - s0 * sk)
            top = sine if k % 2 == 0 else -sine
            near = d == 0.0
            val = jnp.where(near, 1.0, top / jnp.where(near, 1.0, d)) * taper
            keep = (jnp.abs(d) < 4.0) & (col + n >= 0) & (col + n < cols)
            val = jnp.where(keep, val, 0.0)
            weight[g, k] = val.astype(jnp.bfloat16).astype(jnp.float32)


def column(values):
    row = lax.broadcasted_iota(jnp.int32, (len(values), 128), 0)
    made = jnp.zeros((len(values), 128), jnp.asarray(values[0]).dtype)
    for r, value in enumerate(values):
        made = jnp.where(row == r, value, made)
    return made


def azimuth_band(fraction, base, line, blocks):
    held = lax.broadcasted_iota(jnp.int32, (blocks, 128), 1)
    row = jnp.where(held < blocks, held, held - blocks - HALO)
    row = jnp.where(held < blocks + HALO, row, held - HALO)
    gap = row - line - base
    d = gap.astype(jnp.float32) - fraction
    near = d == 0.0
    safe = jnp.where(near, 1.0, d)
    whole = jnp.round(safe)
    sine = jnp.sin(PI * (safe - whole)) * (1 - 2 * (whole.astype(jnp.int32) & 1)).astype(jnp.float32)
    value = jnp.where(near, 1.0, sine / (PI * safe)) * (0.5 + 0.5 * jnp.cos(PI * d / 4.0))
    keep = (jnp.abs(d) < 4.0) & (jnp.abs(gap) <= 4) & (held < blocks + 2 * HALO)
    return jnp.where(keep, value, 0.0).astype(jnp.bfloat16)


def send_order(me, count, i):
    half = count // 2
    mine = me // half
    own = i // half
    side = mine * own + (1 - mine) * (1 - own)
    return side * half + lax.rem(me - mine * half + own + i - own * half, half)


def swath_kernel(
    cuts, coef, shift, dest, valid, first, last, az_coef, az_base, image,
    got, notes,
    held, edge, dense, weight, sent, memo, start, order,
    ready, own_sem, halo_send, halo_recv, edge_send, edge_recv, send_sem, recv_sem, note_send, note_recv,
):
    blocks, cols = image.shape[1], image.shape[2]
    tiles = cols // 128
    span = dense.shape[0] // (2 * blocks)
    count = lax.axis_size("az")
    me = lax.axis_index("az")
    after, before = lax.rem(me + 1, count), lax.rem(me + count - 1, count)
    own = pltpu.make_async_copy(image, held.at[:, pl.ds(0, blocks)], own_sem)
    own.start()

    barrier = pltpu.get_barrier_semaphore()

    for peer in (after, before):
        pl.semaphore_signal(barrier, inc=1, device_id={"az": peer})
    low_edge = [jnp.where(valid[r] > 0, first[r], cols) for r in range(blocks)]
    high_edge = [jnp.where(valid[r] > 0, last[r], 0) for r in range(blocks)]
    edge[0, pl.ds(0, blocks), :] = column(low_edge).astype(jnp.float32)
    edge[1, pl.ds(0, blocks), :] = column(high_edge).astype(jnp.float32)
    pl.semaphore_wait(barrier, 2)

    steps = cols // STEP
    chunks = len(cuts) - 1
    per = steps // (tiles // 16)
    bounds = [0] + [cut * per + 1 for cut in cuts[1:-1]] + [steps]
    ways = ((after, blocks - HALO, blocks), (before, 0, blocks + HALO))
    for w, (peer, source, slot) in enumerate(ways):
        pltpu.make_async_remote_copy(
            src_ref=edge.at[:, pl.ds(source, HALO), :],
            dst_ref=edge.at[:, pl.ds(slot, HALO), :],
            send_sem=edge_send.at[w],
            recv_sem=edge_recv.at[w],
            device_id={"az": peer},
        ).start()
    halo = []
    for c in range(chunks):
        at = pl.ds(bounds[c] * STEP, (bounds[c + 1] - bounds[c]) * STEP)
        for w, (peer, source, slot) in enumerate(ways):
            copy = pltpu.make_async_remote_copy(
                src_ref=image.at[:, pl.ds(source, HALO), at],
                dst_ref=held.at[:, pl.ds(slot, HALO), at],
                send_sem=halo_send.at[c, w],
                recv_sem=halo_recv.at[c, w],
                device_id={"az": peer},
            )
            copy.start()
            halo.append(copy)

    def meet(r):
        for peer in (lax.rem(me + (1 << r), count), lax.rem(me + count - (1 << r), count)):
            pl.semaphore_signal(ready.at[r], inc=1, device_id={"az": peer})

    meetings = ready.shape[0]
    meet(0)
    lines = []
    for i in range(blocks):
        target = send_order(me, count, i)
        line = jnp.int32(0)
        for j in range(blocks):
            line = jnp.where(dest[j] // blocks == target, j, line)
        order[i] = line
        lines.append(line)
    c0 = column([az_coef[0, j] for j in lines])
    c1 = column([az_coef[1, j] for j in lines])
    c2 = column([az_coef[2, j] for j in lines])
    q = 0.5
    fraction = c0 + c1 * q + c2 * q * q
    band = azimuth_band(fraction, column([az_base[j] for j in lines]), column(lines), blocks)
    band = band[:, : blocks + 2 * HALO]
    pl.semaphore_wait(ready.at[0], 2)
    if meetings > 1:
        meet(1)
    range_weights(coef, start, weight, cols)
    for r in range(1, meetings):
        pl.semaphore_wait(ready.at[r], 2)
        if r + 1 < meetings:
            meet(r + 1)

    own.wait()
    for w, (peer, source, slot) in enumerate(ways):
        pltpu.make_async_remote_copy(
            src_ref=edge.at[:, pl.ds(source, HALO), :],
            dst_ref=edge.at[:, pl.ds(slot, HALO), :],
            send_sem=edge_send.at[w],
            recv_sem=edge_recv.at[w],
            device_id={"az": peer},
        ).wait()
    low = edge[0]
    high = edge[1]
    row = lax.broadcasted_iota(jnp.int32, high.shape, 0)
    outside = ((me == 0) & (row >= blocks) & (row < blocks + HALO)) | (
        (me == count - 1) & (row >= blocks + HALO)
    )
    high = jnp.where(outside, 0.0, high)
    lane_held = lax.broadcasted_iota(jnp.int32, high.shape, 1).astype(jnp.float32)
    lane_row = lax.broadcasted_iota(jnp.int32, (blocks, 128), 1)
    lane = lax.broadcasted_iota(jnp.int32, (8, 128), 1)

    def azimuth(s, tails):
        at = pl.ds(pl.multiple_of(s * STEP, STEP), STEP)
        keeps = []
        for u in range(STEP // 128):
            col = lane_held + (s * STEP + u * 128).astype(jnp.float32)
            keeps.append((col >= low) & (col < high))
        new_tails = []
        for p in range(2):
            rows = held[p, :, at].astype(jnp.float32)
            rows = jnp.concatenate(
                [
                    jnp.where(keep, rows[:, u * 128 : u * 128 + 128], 0.0)
                    for u, keep in enumerate(keeps)
                ],
                axis=1,
            ).astype(jnp.bfloat16)
            out = jnp.dot(band, rows, preferred_element_type=jnp.float32)
            out = out.astype(jnp.bfloat16).astype(jnp.float32)
            tail = tails[p]
            for u in range(STEP // 128):
                turned = pltpu.roll(out[:, u * 128 : u * 128 + 128], 64, 1)
                place = p * blocks * span + s * (STEP // 128) + u
                dense[pl.ds(place, blocks, stride=span), :] = jnp.where(lane_row < 64, tail, turned)
                tail = turned
            new_tails.append(tail)
        return tuple(new_tails)

    def filtered(i, big, power):
        for p in range(2):
            halves = []
            for h in range(2):
                g = big * 2 + h
                b = shift[order[i]] + start[g] + 64
                at = pl.multiple_of((p * blocks + i) * span + g * 8, 8)
                x0 = dense[pl.ds(at, 8), :]
                x1 = dense[pl.ds(at + 1, 8), :]
                acc = None
                for k in range(TAPS):
                    moved = pltpu.roll(jnp.where(lane < b + k, x1, x0), 128 - b - k, 1)
                    term = weight[g, k] * moved
                    acc = term if acc is None else acc + term
                halves.append(acc)
            done = jnp.concatenate(halves, axis=0).astype(jnp.bfloat16)
            sent[i, p, pl.ds(pl.multiple_of(big * 16, 16), 16), :] = done
            wide = done.astype(jnp.float32)
            power = power + wide * wide
        return power

    tails = (jnp.zeros((blocks, 128), jnp.float32),) * 2
    power = jnp.zeros((16, 128), jnp.float32)
    for c in range(chunks):
        for copy in halo[2 * c : 2 * c + 2]:
            copy.wait()
        tails = lax.fori_loop(bounds[c], bounds[c + 1], azimuth, tails)
        if c == chunks - 1:
            for p in range(2):
                ends = jnp.where(lane_row < 64, tails[p], 0.0)
                dense[pl.ds(p * blocks * span + tiles, blocks, stride=span), :] = ends
        lo, hi = cuts[c], cuts[c + 1]
        at = pl.ds(lo * 16, (hi - lo) * 16)

        def line(i, power):
            power = lax.fori_loop(lo, hi, functools.partial(filtered, i), power, unroll=True)

            @pl.when(i < count - 1)
            def _():
                pltpu.make_async_remote_copy(
                    src_ref=sent.at[i, :, at, :],
                    dst_ref=got.at[me, :, at, :],
                    send_sem=send_sem.at[c, i],
                    recv_sem=recv_sem.at[c, me],
                    device_id={"az": send_order(me, count, i)},
                ).start()

            return power

        power = lax.fori_loop(0, blocks, line, power)

    own_power = jnp.broadcast_to(jnp.sum(power, keepdims=True), (NOTE, 128))
    have = jnp.int32(0)
    for j in range(blocks):
        have = have + jnp.maximum(
            jnp.minimum(high_edge[j], cols) - jnp.maximum(low_edge[j], 0), 0
        )
    own_count = jnp.full((NOTE, 128), have, jnp.int32).astype(jnp.float32)
    row = lax.broadcasted_iota(jnp.int32, (NOTE, 128), 0)
    stats = jnp.where(row == 1, own_power, own_count)
    for i in range(blocks):
        place = jnp.full((NOTE, 128), dest[lines[i]] % blocks, jnp.int32).astype(jnp.float32)
        memo[i] = jnp.where(row == 0, place, stats)

    def tell(i, carry):
        pltpu.make_async_remote_copy(
            src_ref=memo.at[i],
            dst_ref=notes.at[me],
            send_sem=note_send.at[i],
            recv_sem=note_recv.at[me],
            device_id={"az": send_order(me, count, i)},
        ).start()
        return carry

    lax.fori_loop(0, count - 1, tell, 0)
    notes[me] = memo[blocks - 1]
    got[me] = sent[blocks - 1]

    def take(i, carry):
        peer = send_order(me, count, i)
        for c in range(chunks):
            lo, hi = cuts[c], cuts[c + 1]
            at = pl.ds(lo * 16, (hi - lo) * 16)
            done = pltpu.make_async_remote_copy(
                src_ref=sent.at[i, :, at, :],
                dst_ref=got.at[peer, :, at, :],
                send_sem=send_sem.at[c, i],
                recv_sem=recv_sem.at[c, peer],
                device_id={"az": peer},
            )
            done.wait_send()
            done.wait_recv()
        told = pltpu.make_async_remote_copy(
            src_ref=memo.at[i],
            dst_ref=notes.at[peer],
            send_sem=note_send.at[i],
            recv_sem=note_recv.at[peer],
            device_id={"az": peer},
        )
        told.wait_send()
        told.wait_recv()
        return carry

    lax.fori_loop(0, count - 1, take, 0)


def finish_kernel(total, got, notes, out, mean, share, wide):
    blocks, cols = out.shape[1], out.shape[2]
    tiles = cols // 128
    told = [notes[s] for s in range(blocks)]
    both = functools.reduce(lambda a, b: a + b, told)
    power, count = both[1:2], both[2:3]
    mean_power = power / jnp.maximum(count, 1.0)
    gain = lax.rsqrt(mean_power + 0.5)
    mean[0] = mean_power[0, 0]
    share[0] = (count / float(total))[0, 0]
    for s in range(blocks):
        place = told[s][0, 0].astype(jnp.int32)
        for p in range(2):
            x = got[s, p].astype(jnp.float32) * gain
            wide[pl.ds(pl.multiple_of((p * blocks + place) * tiles, 8), tiles), :] = x
    for t in range(tiles):
        for p in range(2):
            x = wide[pl.ds(p * blocks * tiles + t, blocks, stride=tiles), :]
            out[p, :, t * 128 : t * 128 + 128] = x.astype(jnp.bfloat16)


def shards(
    secondary, line_valid, first_valid, last_valid, az_coef, az_base, rg_base, rg_coef, block_dest
):
    cols = secondary.shape[2]
    blocks = block_dest.shape[0]
    tiles = cols // 128
    count = lax.axis_size("az")
    bigs = tiles // 16
    cuts = [0] + sorted({bigs * cut // 6 for cut in CUTS} - {0, bigs}) + [bigs]
    chunks = len(cuts) - 1
    parts = max(c for c in range(1, PARTS + 1) if bigs % c == 0)
    smem = pl.BlockSpec(memory_space=pltpu.SMEM)
    vmem = pl.BlockSpec(memory_space=pltpu.VMEM)
    held = blocks + 2 * HALO
    dma = pltpu.SemaphoreType.DMA
    got, notes = pl.pallas_call(
        functools.partial(swath_kernel, cuts),
        out_shape=(
            jax.ShapeDtypeStruct((blocks, 2, tiles, 128), jnp.bfloat16),
            jax.ShapeDtypeStruct((blocks, NOTE, 128), jnp.float32),
        ),
        in_specs=[smem] * 8 + [pl.BlockSpec(memory_space=pl.ANY)],
        out_specs=(vmem, vmem),
        scratch_shapes=[
            pltpu.VMEM((2, held, cols), jnp.bfloat16),
            pltpu.VMEM((2, held, 128), jnp.float32),
            pltpu.VMEM((2 * blocks * (tiles + 8), 128), jnp.float32),
            pltpu.VMEM((tiles // 8, TAPS, 8, 128), jnp.float32),
            pltpu.VMEM((blocks, 2, tiles, 128), jnp.bfloat16),
            pltpu.VMEM((blocks, NOTE, 128), jnp.float32),
            pltpu.SMEM((tiles // 8,), jnp.int32),
            pltpu.SMEM((blocks,), jnp.int32),
            pltpu.SemaphoreType.REGULAR((max(1, (count // 2 - 1).bit_length()),)),
            dma(()),
            dma((chunks, 2)),
            dma((chunks, 2)),
            dma((2,)),
            dma((2,)),
            dma((chunks, blocks)),
            dma((chunks, blocks)),
            dma((blocks,)),
            dma((blocks,)),
        ],
        compiler_params=pltpu.CompilerParams(collective_id=0, has_side_effects=True),
        name="swath",
    )(
        rg_coef, rg_base, block_dest, line_valid, first_valid, last_valid, az_coef, az_base,
        secondary,
    )
    return pl.pallas_call(
        functools.partial(finish_kernel, cols * blocks * count),
        out_shape=(
            jax.ShapeDtypeStruct((2, blocks, cols), jnp.bfloat16),
            jax.ShapeDtypeStruct((1,), jnp.float32),
            jax.ShapeDtypeStruct((1,), jnp.float32),
        ),
        grid=(parts,),
        in_specs=[pl.BlockSpec((blocks, 2, tiles // parts, 128), lambda c: (0, 0, c, 0)), vmem],
        out_specs=(pl.BlockSpec((2, blocks, cols // parts), lambda c: (0, 0, c)), smem, smem),
        scratch_shapes=[pltpu.VMEM((2 * blocks * (tiles // parts), 128), jnp.float32)],
        name="finish",
    )(got, notes)


CUTS = (2,)
PARTS = 2


def solution(mesh):
    rows = P(("scene", "az"))
    placed = (
        P(None, ("scene", "az"), None),
        rows,
        rows,
        rows,
        P(None, ("scene", "az")),
        rows,
        rows,
        P("scene"),
        rows,
    )
    return jax.shard_map(
        shards,
        mesh=mesh,
        in_specs=placed,
        out_specs=(P(None, ("scene", "az"), None), P("scene"), P("scene")),
        check_vma=False,
    )
```
